256 devices in a mesh: seq: 32 (over y, x, core), tensor: 8 (over z).
Axes of the slice: x: 4, y: 4, z: 8, core: 2. Of those that a mesh axis runs over, the one named last changes fastest.
Arguments:
- streams: float32 [4, 16384, 4096], P(None, 'seq', 'tensor'), may hold values from -8 to 8
- mix_weight: float32 [24, 4, 4096], P(None, None, 'tensor'), may hold values from -0.046875 to 0.046875
- mix_bias: float32 [24], replicated, may hold values from -4 to 4
- mix_scale: float32 [3], replicated, may hold values from 1 to 2
- norm_gain: bfloat16 [4096], replicated, may hold values from 0.25 to 1.75
- gate_weight: bfloat16 [4096, 7168], P('seq', 'tensor'), may hold values from -0.09375 to 0.09375
- up_weight: bfloat16 [4096, 7168], P('seq', 'tensor'), may hold values from -0.09375 to 0.09375
- down_weight: bfloat16 [7168, 4096], P('tensor', 'seq'), may hold values from -0.0625 to 0.0625
Outputs:
- new_streams: float32 [4, 16384, 4096], P(None, 'seq', 'tensor')
The draws below stay inside these ranges and needn't reach their ends.
All inputs are finite; a program needn't handle non-finite values.
Results may differ from the reference program's by a relative error of at most 0.01.
Values may be sent and summed in bfloat16 or wider, within the bound.
No kernel may reach another device: no remote copies, remote signals or barrier semaphores. Data moves between devices by JAX's collectives and lax.ppermute only.
A program may use at most 128 MiB of HBM per device.

```python
import jax
import jax.numpy as jnp
from jax import lax

D = 4096
FF = 7168
STREAMS = 4
SWEEPS = 20
TOK_DEV = 512
TOKENS = 16384
LOGITS = 24
N_SEQ = 32
N_TENSOR = 8


def draw_streams(key, part):
    first = jax.random.fold_in(key, 11)
    second = jax.random.fold_in(key, 12)
    fifth = jax.random.fold_in(key, 15)
    groups = max(D // 64, 1)
    columns = D // groups
    scales = jnp.exp(jax.random.uniform(second, (STREAMS, TOKENS, groups, 1), jnp.float32, -1.2, 1.2))
    coarse = jnp.exp(jax.random.uniform(fifth, (STREAMS, TOKENS, 8, 1), jnp.float32, -1.5, 1.5))
    values = jax.random.normal(first, (STREAMS, TOKENS, groups, columns), jnp.float32) * scales
    values = values.reshape(STREAMS, TOKENS, 8, D // 8) * coarse
    return jnp.clip(values, -8.0, 8.0).reshape(STREAMS, TOKENS, D)


def steps_of(stream_key, dims, shards, least, high):
    level, own = 1.0, jax.random.fold_in(stream_key, 6)
    for dim, blocks in shards:
        steps = jnp.exp(jax.random.uniform(jax.random.fold_in(own, dim), (blocks,), jnp.float32, least / len(shards), high / len(shards)))
        level = level * jnp.repeat(steps, dims[dim] // blocks).reshape([-1 if axis == dim else 1 for axis in range(len(dims))])
    return level


def noise(own_key, shape, scale, bound, cuts=(), kind=jnp.bfloat16):
    array = scale * jax.random.normal(own_key, shape, jnp.float32)
    if cuts:
        array = array * steps_of(own_key, shape, cuts, -0.22, 0.18)
    return jnp.clip(array, -bound, bound).astype(kind)


def setup_inputs(seed: int = 0) -> dict:
    keys = jax.random.split(jax.random.key(seed), 9)
    return {
        "streams": draw_streams(jax.random.fold_in(keys[8], 71), 0),
        "mix_weight": noise(keys[1], (LOGITS, STREAMS, D), (STREAMS * D) ** -0.5, 0.046875, ((2, 8),), jnp.float32),
        "mix_bias": noise(keys[2], (LOGITS,), 1.0, 4.0, (), jnp.float32),
        "mix_scale": jnp.clip(jax.random.uniform(keys[3], (3,), jnp.float32, 1.0, 2.0), 1.0, 2.0),
        "norm_gain": jnp.clip(1.0 + 0.15 * jax.random.normal(keys[4], (D,), jnp.float32), 0.25, 1.75).astype(jnp.bfloat16),
        "gate_weight": noise(keys[5], (D, FF), D ** -0.5, 0.09375, ((0, 32), (1, 8))),
        "up_weight": noise(keys[6], (D, FF), D ** -0.5, 0.09375, ((0, 32), (1, 8))),
        "down_weight": noise(keys[7], (FF, D), FF ** -0.5, 0.0625, ((0, 8), (1, 32))),
    }


epsilon = 0.25

def coefficients(logits, mix_bias, mix_scale):
    pre_mix = jax.nn.sigmoid(mix_scale[0] * logits[:STREAMS] + mix_bias[:STREAMS, None])
    post_mix = 2.0 * jax.nn.sigmoid(mix_scale[1] * logits[STREAMS:2 * STREAMS] + mix_bias[STREAMS:2 * STREAMS, None])
    start_mix = jnp.exp(mix_scale[2] * logits[2 * STREAMS:] + mix_bias[2 * STREAMS:, None])
    start_mix = start_mix.reshape(STREAMS, STREAMS, logits.shape[1])

    def balance(iteration, matrix):
        matrix = matrix / lax.optimization_barrier(jnp.sum(matrix, axis=1, keepdims=True))
        return matrix / lax.optimization_barrier(jnp.sum(matrix, axis=0, keepdims=True))
    return (pre_mix, post_mix, lax.fori_loop(0, SWEEPS, balance, start_mix))

def layer_block(block, streams, mix_weight, mix_bias, mix_scale, norm_gain, gate_weight, up_weight, down_weight):
    current = lax.dynamic_slice_in_dim(streams, (block * TOK_DEV).astype(jnp.int32), TOK_DEV, 1)
    squares = lax.optimization_barrier(jnp.sum(current * current, axis=(0, 2)))
    inverse = lax.rsqrt(squares / (STREAMS * D) + epsilon)
    raw_logits = jnp.einsum('lkd,ktd->lt', mix_weight, current, precision=lax.Precision.HIGHEST)
    pre_mix, post_mix, res_mix = coefficients(raw_logits * inverse[None, :], mix_bias, mix_scale)
    layer_in = lax.optimization_barrier(jnp.sum(pre_mix[:, :, None] * current, axis=0)).astype(jnp.bfloat16)
    as_float = layer_in.astype(jnp.float32)
    mean_square = lax.optimization_barrier(jnp.mean(as_float * as_float, axis=1, keepdims=True))
    normed = (as_float * lax.rsqrt(mean_square + epsilon) * norm_gain.astype(jnp.float32)).astype(jnp.bfloat16)
    gate_value = jnp.dot(normed, gate_weight, preferred_element_type=jnp.float32)
    up_value = jnp.dot(normed, up_weight, preferred_element_type=jnp.float32)
    hidden = (jax.nn.silu(gate_value) * up_value).astype(jnp.bfloat16)
    share = FF // N_TENSOR
    layer_out = jnp.zeros((TOK_DEV, D), jnp.float32)
    for group in range(N_TENSOR):
        partial_out = jnp.dot(hidden[:, group * share:(group + 1) * share], down_weight[group * share:(group + 1) * share], preferred_element_type=jnp.float32)
        rounded = lax.optimization_barrier(partial_out.astype(jnp.bfloat16))
        layer_out = layer_out + rounded.astype(jnp.float32)
    outputs = []
    for target in range(STREAMS):
        mixed = post_mix[target][:, None] * layer_out
        for source in range(STREAMS):
            mixed = mixed + res_mix[target, source][:, None] * current[source]
        outputs.append(mixed)
    return jnp.stack(outputs)

def reference(streams, mix_weight, mix_bias, mix_scale, norm_gain, gate_weight, up_weight, down_weight):

    def one_block(block):
        return layer_block(block, streams, mix_weight, mix_bias, mix_scale, norm_gain, gate_weight, up_weight, down_weight)
    blocks = lax.map(one_block, jnp.arange(N_SEQ, dtype=jnp.int32))
    return jnp.moveaxis(blocks, 0, 1).reshape(STREAMS, TOKENS, D)
```

```python
import functools

import jax
import jax.numpy as jnp
from jax import lax
from jax.experimental import pallas as pl
from jax.experimental.pallas import tpu as pltpu
from jax.sharding import PartitionSpec as P

D = 4096
STREAMS = 4
SWEEPS = 20
TOK = 512
HALF = 256
FEAT = 512
HID = 896
ROWS = 128

epsilon = 0.25
bf16, f32 = jnp.bfloat16, jnp.float32


def seq_pairs(phase, step):
    pairs = []
    for s in range(32):
        y, x, c = s // 8, s // 2 % 4, s % 2
        if (phase == 1) == (c == 0):
            x = (x + step) % 4
        else:
            y = (y + step) % 4
        pairs.append((s, 8 * y + 2 * x + c))
    return pairs


P1P, P1M, P2P, P2M = seq_pairs(1, 1), seq_pairs(1, -1), seq_pairs(2, 1), seq_pairs(2, -1)
SWAP = [(s, s ^ 1) for s in range(32)]


def ring(step):
    return [(i, (i + step) % 8) for i in range(8)]


def over_seq(value, pairs):
    return lax.ppermute(value, "seq", pairs)


def over_tensor(value, step):
    return lax.ppermute(value, "tensor", ring(step))


def cost(flops, nbytes):
    return pl.CostEstimate(flops=int(flops), bytes_accessed=int(nbytes), transcendentals=0)


PIECES = ((0, 0), (0, 1), (3, 0), (3, 1), (1, 0), (1, 1), (2, 0), (2, 1))


def gather_plane(shard):
    rows = shard.shape[0]
    minus = over_seq(shard, P1P)
    plus = over_seq(shard, P1M)
    far_a = over_seq(minus[: rows // 2], P1P)
    far_b = over_seq(plus[rows // 2 :], P1M)
    a = jnp.concatenate([shard, plus])
    b = jnp.concatenate([far_a, far_b, minus])
    minus_a, minus_b = over_seq(a, P2P), over_seq(b, P2P)
    plus_b, plus_a = over_seq(b, P2M), over_seq(a, P2M)
    far_a, far_b = over_seq(minus_a, P2P), over_seq(plus_b, P2M)
    own = [a, b, minus_a, minus_b, plus_a, plus_b, far_a, far_b]
    return own + [over_seq(piece, SWAP) for piece in own]


def seq_shard(pos, number, item):
    rel2, part = PIECES[number % 8]
    rel1 = 2 * part + item
    y, x, c = pos[0], pos[1], pos[2]
    core = c if number < 8 else 1 - c
    first = core == 0
    a = (jnp.where(first, x, y) + rel1) & 3
    b = (jnp.where(first, y, x) + rel2) & 3
    return 8 * jnp.where(first, b, a) + 2 * jnp.where(first, a, b) + core


def stats_kernel(streams, weight, out, out16):
    total = jnp.zeros((24, ROWS), f32)
    squares = jnp.zeros((ROWS, FEAT), f32)
    for k in range(STREAMS):
        s = streams[k]
        squares += s * s
        total += lax.dot_general(
            weight[:, k, :].astype(bf16), s.astype(bf16), (((1,), (1,)), ((), ())), preferred_element_type=f32
        )
    norm = lax.dot_general(
        jnp.ones((8, FEAT), bf16), squares.astype(bf16), (((1,), (1,)), ((), ())), preferred_element_type=f32
    )
    out[:24, :] = total
    out[24:, :] = norm
    out16[:24, :] = total.astype(bf16)
    out16[24:, :] = norm.astype(bf16)


def stats(streams, weight):
    return pl.pallas_call(
        stats_kernel,
        grid=(4,),
        in_specs=[
            pl.BlockSpec((STREAMS, ROWS, FEAT), lambda i: (0, i, 0)),
            pl.BlockSpec((24, STREAMS, FEAT), lambda i: (0, 0, 0)),
        ],
        out_specs=[pl.BlockSpec((32, ROWS), lambda i: (0, i))] * 2,
        out_shape=[jax.ShapeDtypeStruct((32, TOK), f32), jax.ShapeDtypeStruct((32, TOK), bf16)],
        cost_estimate=cost(2e9, 4.2e6),
        name="stats",
    )(streams, weight)


def window_kernel(own, left, right, three, three16, two16):
    two = own[...] + left[...].astype(f32)
    both = two + right[...].astype(f32)
    three[...] = both
    three16[...] = both.astype(bf16)
    two16[...] = two.astype(bf16)


def window(own, left, right):
    return pl.pallas_call(
        window_kernel,
        out_shape=[jax.ShapeDtypeStruct((32, TOK), t) for t in (f32, bf16, bf16)],
        cost_estimate=cost(1e8, 2e5),
        name="window",
    )(own, left, right)


def logits_of(three, left, right):
    total = three[...] + left[...].astype(f32) + right[...].astype(f32)
    inverse = lax.rsqrt(total[24:25] / (STREAMS * D) + epsilon)
    return total[:24] * inverse


def layer_kernel(three, left, right, scale, bias, streams, out):
    logits = logits_of(three, left, right)
    mix = jax.nn.sigmoid(scale[:8] * logits[:8] + bias[:8])
    columns = jnp.transpose(mix)
    total = columns[:, 0:1] * streams[0]
    for k in range(1, STREAMS):
        total += columns[:, k : k + 1] * streams[k]
    out[...] = total.astype(bf16)


def layer_input(three, left, right, scale, bias, streams, half):
    small = pl.BlockSpec((32, ROWS), lambda i: (0, 2 * half + i))
    whole = pl.BlockSpec((24, 1), lambda i: (0, 0))
    return pl.pallas_call(
        layer_kernel,
        grid=(2,),
        in_specs=[small, small, small, whole, whole]
        + [pl.BlockSpec((STREAMS, ROWS, FEAT), lambda i: (0, 2 * half + i, 0))],
        out_specs=pl.BlockSpec((ROWS, FEAT), lambda i: (i, 0)),
        out_shape=jax.ShapeDtypeStruct((HALF, FEAT), bf16),
        cost_estimate=cost(1e9, 2.4e6),
        name="layer_input",
    )(three, left, right, scale, bias, streams)


def coefficients_kernel(three, left, right, scale, bias, out):
    logits = logits_of(three, left, right)
    value = scale[...] * logits + bias[...]
    post = 2.0 * jax.nn.sigmoid(value[4:8])
    start = jnp.exp(value[8:]).reshape(STREAMS, STREAMS, TOK)

    def balance(_, matrix):
        matrix = matrix / jnp.sum(matrix, axis=1, keepdims=True)
        return matrix / jnp.sum(matrix, axis=0, keepdims=True)

    res = lax.fori_loop(0, SWEEPS, balance, start)
    rows = [post] + [res[k] for k in range(STREAMS)] + [jnp.zeros((108, TOK), f32)]
    out[...] = jnp.transpose(jnp.concatenate(rows, axis=0))


def coefficients(three, left, right, scale, bias):
    return pl.pallas_call(
        coefficients_kernel,
        out_shape=jax.ShapeDtypeStruct((TOK, 128), f32),
        cost_estimate=cost(2e9, 4e5),
        name="coefficients",
    )(three, left, right, scale, bias)


def project_kernel(blocks, last, n_tok, *refs):
    pos = refs[0]
    tokens = refs[1 : 1 + n_tok]
    pieces = refs[1 + n_tok : 17 + n_tok]
    refs = refs[17 + n_tok :]
    if last:
        before, before_sq, out, wv, acc, sems = refs
    else:
        acc, out_sq, wv, sems = refs
    z = pos[3]
    for number in range(16):
        for item in range(2):
            s = seq_shard(pos, number, item)
            rel = ((s >> 2) - z) & 7
            slot = jnp.int32(-1)
            for n, (k, _) in enumerate(blocks):
                slot = jnp.where(rel == k, n, slot)

            @pl.when(slot >= 0)
            def _():
                pltpu.make_async_copy(
                    pieces[number].at[pl.ds(item * ROWS, ROWS), :],
                    wv.at[slot, pl.ds(pl.multiple_of((s & 3) * ROWS, ROWS), ROWS), :],
                    sems.at[slot],
                ).start()

    squares = before_sq[...] if last else jnp.zeros((TOK, 128), f32)
    for n, (k, parts) in enumerate(blocks):
        for q in range(4):
            pltpu.make_async_copy(
                pieces[0].at[pl.ds(0, ROWS), :], wv.at[n, pl.ds(q * ROWS, ROWS), :], sems.at[n]
            ).wait()
        x = jnp.concatenate([tokens[p][...] for p in parts], axis=0)
        xf = x.astype(f32)
        xf = xf * xf
        for q in range(4):
            squares += xf[:, q * 128 : (q + 1) * 128]
        product = jnp.dot(x, wv[n], preferred_element_type=f32)
        if n:
            acc[...] += product
        elif last:
            acc[...] = before[...] + product
        else:
            acc[...] = product
    if not last:
        out_sq[...] = squares
    else:
        factor = lax.rsqrt(jnp.sum(squares, axis=1, keepdims=True) / D + epsilon)
        gate = acc[:, :HID] * factor
        up = acc[:, HID:] * factor
        out[...] = (gate / (1.0 + jnp.exp(-gate)) * up).astype(bf16)


VMEM = pl.BlockSpec(memory_space=pltpu.VMEM)
ANY = pl.BlockSpec(memory_space=pl.ANY)
SMEM = pl.BlockSpec(memory_space=pltpu.SMEM)


def project(pos, blocks, pieces, before=None):
    last = before is not None
    tokens, plan = [], []
    for k, halves in blocks:
        plan.append((k, (len(tokens), len(tokens) + 1)))
        tokens += list(halves)
    count = len(blocks)
    scratch = [pltpu.VMEM((count, FEAT, 2 * HID), bf16)]
    if last:
        out_shape = jax.ShapeDtypeStruct((TOK, HID), bf16)
        scratch.append(pltpu.VMEM((TOK, 2 * HID), f32))
    else:
        out_shape = [jax.ShapeDtypeStruct((TOK, 2 * HID), f32), jax.ShapeDtypeStruct((TOK, 128), f32)]
    scratch.append(pltpu.SemaphoreType.DMA((count,)))
    return pl.pallas_call(
        functools.partial(project_kernel, plan, last, len(tokens)),
        in_specs=[SMEM] + [VMEM] * len(tokens) + [ANY] * 16 + [VMEM] * (2 if last else 0),
        out_specs=VMEM if last else [VMEM, VMEM],
        out_shape=out_shape,
        scratch_shapes=scratch,
        cost_estimate=cost(2.0 * TOK * FEAT * 2 * HID * count, 1.9e6 * count + 8e6),
        compiler_params=pltpu.CompilerParams(vmem_limit_bytes=56 << 20),
        name="project_last" if last else "project_first",
    )(pos, *tokens, *pieces, *(before if last else ()))


def down_kernel(dests, halves, n_add, n_out, *refs):
    pos, hidden = refs[0], refs[1]
    adds = refs[2 : 2 + n_add]
    pieces = refs[2 + n_add : 18 + n_add]
    outs = refs[18 + n_add : 18 + n_add + n_out]
    wv, sems = refs[18 + n_add + n_out :]
    z = pos[3]
    for number in range(16):
        for item in range(2):
            s = seq_shard(pos, number, item)
            rel = ((s >> 2) - z) & 7
            slot = jnp.int32(-1)
            for n, k in enumerate(dests):
                slot = jnp.where(rel == k, n, slot)

            @pl.when(slot >= 0)
            def _():
                pltpu.make_async_copy(
                    pieces[number].at[pl.ds(item * HID, HID), :],
                    wv.at[slot, :, pl.ds(pl.multiple_of((s & 3) * ROWS, ROWS), ROWS)],
                    sems.at[slot],
                ).start()

    waited = []
    for n, half in enumerate(halves):
        slot = n if len(dests) > n else len(dests) - 1
        if slot not in waited:
            waited.append(slot)
            for q in range(4):
                pltpu.make_async_copy(
                    pieces[0].at[pl.ds(0, HID), :], wv.at[slot, :, pl.ds(q * ROWS, ROWS)], sems.at[slot]
                ).wait()
        value = jnp.dot(
            hidden[half * HALF : (half + 1) * HALF, :], wv[slot], preferred_element_type=f32
        )
        if n_add:
            value += adds[n][...].astype(f32)
        outs[n][...] = value.astype(outs[n].dtype)


def down(pos, hidden, pieces, dests, halves, adds=(), dtype=bf16):
    return pl.pallas_call(
        functools.partial(down_kernel, dests, halves, len(adds), len(halves)),
        in_specs=[SMEM, VMEM] + [VMEM] * len(adds) + [ANY] * 16,
        out_specs=[VMEM] * len(halves),
        out_shape=[jax.ShapeDtypeStruct((HALF, FEAT), dtype)] * len(halves),
        scratch_shapes=[pltpu.VMEM((len(dests), HID, FEAT), bf16), pltpu.SemaphoreType.DMA((len(dests),))],
        cost_estimate=cost(4.0 * HALF * FEAT * HID, 4e6),
        name="down",
    )(pos, hidden, *adds, *pieces)


def final_kernel(own_a, own_b, right_a, left_a, right_b, left_b, coef, streams, out):
    step = pl.program_id(0)

    def mix(own, right, left):
        rows = pl.ds(pl.multiple_of((step & 1) * ROWS, ROWS), ROWS)
        layer_out = own[rows, :] + right[rows, :].astype(f32) + left[rows, :].astype(f32)
        c = coef[...]
        for target in range(STREAMS):
            mixed = c[:, target : target + 1] * layer_out
            for source in range(STREAMS):
                n = STREAMS + STREAMS * target + source
                mixed += c[:, n : n + 1] * streams[source]
            out[target] = mixed

    pl.when(step < 2)(lambda: mix(own_a, right_a, left_a))
    pl.when(step >= 2)(lambda: mix(own_b, right_b, left_b))


def final(own, right_a, left_a, right_b, left_b, coef, streams):
    whole = pl.BlockSpec((HALF, FEAT), lambda i: (0, 0))
    block = pl.BlockSpec((STREAMS, ROWS, FEAT), lambda i: (0, i, 0))
    return pl.pallas_call(
        final_kernel,
        grid=(4,),
        in_specs=[whole] * 6 + [pl.BlockSpec((ROWS, 128), lambda i: (i, 0)), block],
        out_specs=block,
        out_shape=jax.ShapeDtypeStruct((STREAMS, TOK, FEAT), f32),
        cost_estimate=cost(1e9, 1e7),
        name="final",
    )(*own, right_a, left_a, right_b, left_b, coef, streams)


def body(streams, mix_weight, mix_bias, mix_scale, norm_gain, gate_weight, up_weight, down_weight):
    s, z = lax.axis_index("seq"), lax.axis_index("tensor")
    pos = jnp.stack([s // 8, s // 2 % 4, s % 2, z]).astype(jnp.int32)
    gain = lax.dynamic_slice_in_dim(norm_gain, s * ROWS, ROWS).astype(f32)[:, None]
    gate_up = (jnp.concatenate([gate_weight, up_weight], axis=1).astype(f32) * gain).astype(bf16)

    gu = gather_plane(gate_up)
    dn = gather_plane(down_weight)

    own, own16 = stats(streams, mix_weight)
    left, right = over_tensor(own16, 1), over_tensor(own16, -1)
    three, three16, two16 = window(own, left, right)
    left, right = over_tensor(three16, 3), over_tensor(two16, -3)
    scale = jnp.concatenate([jnp.full((4,), mix_scale[0]), jnp.full((4,), mix_scale[1]), jnp.full((16,), mix_scale[2])])
    scale, bias = scale[:, None], mix_bias[:, None]
    a = layer_input(three, left, right, scale, bias, streams, 0)
    b = layer_input(three, left, right, scale, bias, streams, 1)
    coef = coefficients(three, left, right, scale, bias)

    blocks = {0: (a, b)}
    ra, la, rb, lb = a, a, b, b
    for k in (1, 2, 3):
        ra, la = over_tensor(ra, 1), over_tensor(la, -1)
        rb, lb = over_tensor(rb, 1), over_tensor(lb, -1)
        blocks[8 - k], blocks[k] = (ra, rb), (la, lb)
    blocks[4] = (over_tensor(ra, 1), over_tensor(lb, -1))
    before = project(pos, [(k, blocks[k]) for k in (0, 7, 1, 6, 2)], gu)
    hidden = project(pos, [(k, blocks[k]) for k in (5, 3, 4)], gu, before)

    r4a, l4b = down(pos, hidden, dn, (4,), (0, 1))
    r4a, l4b = over_tensor(r4a, 1), over_tensor(l4b, -1)
    r3b, l3a = down(pos, hidden, dn, (3, 5), (1, 0))
    r3b, l3a = over_tensor(r3b, 1), over_tensor(l3a, -1)
    ra, lb, rb, la = r4a, l4b, r3b, l3a
    for k in (3, 2, 1):
        ra, lb = down(pos, hidden, dn, (k, 8 - k), (0, 1), (ra, lb))
        ra, lb = over_tensor(ra, 1), over_tensor(lb, -1)
        if k > 1:
            rb, la = down(pos, hidden, dn, (k - 1, 9 - k), (1, 0), (rb, la))
            rb, la = over_tensor(rb, 1), over_tensor(la, -1)
    mine = down(pos, hidden, dn, (0,), (0, 1), (), f32)
    return final(mine, ra, la, rb, lb, coef, streams)


def solution(mesh):
    placed = (
        P(None, "seq", "tensor"),
        P(None, None, "tensor"),
        P(),
        P(),
        P(),
        P("seq", "tensor"),
        P("seq", "tensor"),
        P("tensor", "seq"),
    )
    return jax.shard_map(
        body, mesh=mesh, in_specs=placed, out_specs=P(None, "seq", "tensor"), check_vma=False
    )
```
